32 devices in a mesh: dev: 4 (over y, x), ma: 8 (over z, core).
Axes of the slice: x: 2, y: 2, z: 4, core: 2. Of those that a mesh axis runs over, the one named last changes fastest.
Arguments:
- joined_weight: bfloat16 [8, 4096, 6144], P(None, 'dev', 'ma'), may hold values from -6 to 6
- norm_gain: float32 [8, 4096], P(None, 'ma'), may hold values from 0.5 to 1.5
- rotary_order: int32 [128], replicated, may hold values from 0 to 127, each once
Outputs:
- query_weight: bfloat16 [8, 4096, 4096], P(None, 'dev', 'ma')
- key_weight: bfloat16 [8, 1024, 4096], P(None, 'dev', 'ma')
- value_weight: bfloat16 [8, 1024, 4096], P(None, 'dev', 'ma')
- row_peak: float32 [8, 6144], P(None, 'dev')
The draws below stay inside these ranges and needn't reach their ends.
Inputs may be any that keep to these rules, and one draw needn't show every extreme that they name: rotary_order holds every number of 0 to 127 exactly once.
All inputs are finite; a program needn't handle non-finite values.
Results may differ from the reference program's by a relative error of at most 0.0055.
Values may be sent and summed in bfloat16 or wider, within the bound.
A program may use at most 256 MiB of HBM per device.

```python
import jax
import jax.numpy as jnp

D = 4096
HEADS = 32
KV_HEADS = 8
HEAD_DIM = 128
LAYERS = 8
GROUP = 4
QKV_COLS = 6144


def shard_levels(stream_key, shape, pieces, low, top_value):
    def one(position, parts):
        steps = jax.random.uniform(jax.random.fold_in(jax.random.fold_in(stream_key, 6), position), (parts,), jnp.float32, low / len(pieces), top_value / len(pieces))
        return jnp.repeat(jnp.exp(steps), shape[position] // parts).reshape((-1,) + (1,) * (len(shape) - position - 1))

    level = one(*pieces[0])
    for cut in pieces[1:]:
        level = level * one(*cut)
    return level


def bell_draw(stream_key, extent, width, reach, cuts=(), kind=jnp.bfloat16):
    drawn = jax.random.normal(stream_key, extent, jnp.float32) * width
    if len(cuts) > 0:
        drawn = shard_levels(stream_key, extent, cuts, -0.22, 0.18) * drawn
    return jnp.clip(drawn, min=-reach, max=reach).astype(kind)


def setup_inputs(seed: int = 0) -> dict:
    keys = jax.random.split(jax.random.key(seed), 4)
    return {
        "joined_weight": bell_draw(keys[0], (LAYERS, D, QKV_COLS), 1.0, 6.0, ((1, 4), (2, 8))),
        "norm_gain": jnp.clip(1.0 + 0.1 * jax.random.normal(keys[1], (LAYERS, D), jnp.float32), 0.5, 1.5),
        "rotary_order": jax.random.permutation(keys[2], HEAD_DIM).astype(jnp.int32),
    }


def arrange_whole(stored_layer):
    head_total = HEADS + 2 * KV_HEADS
    split = stored_layer.reshape(1, D, HEAD_DIM, head_total)
    slots_query = split[..., :HEADS].reshape(1, D, HEAD_DIM, KV_HEADS, GROUP)
    slots_key = split[..., HEADS:HEADS + KV_HEADS][..., None]
    slots_value = split[..., HEADS + KV_HEADS:][..., None]
    grouped = jnp.concatenate([slots_query, slots_key, slots_value], axis=4)
    return jnp.transpose(grouped, (0, 3, 4, 2, 1))


def finish_tiles(canonical, gain_rows, rotary_order):
    layer_count = canonical.shape[0]
    column_count = canonical.shape[4]
    turned = jnp.take(canonical[:, :, :GROUP + 1], rotary_order, axis=3)
    complete = jnp.concatenate([turned, canonical[:, :, GROUP + 1:]], axis=2)
    scaled = (complete.astype(jnp.float32) * gain_rows[:, None, None, None, :]).astype(jnp.bfloat16)
    query_rows = scaled[:, :, :GROUP].reshape(layer_count, -1, column_count)
    key_rows = scaled[:, :, GROUP].reshape(layer_count, -1, column_count)
    value_rows = scaled[:, :, GROUP + 1].reshape(layer_count, -1, column_count)
    local_peak = jnp.max(jnp.abs(scaled.astype(jnp.float32)), axis=4).reshape(layer_count, -1)
    return query_rows, key_rows, value_rows, local_peak


def reference(joined_weight, norm_gain, rotary_order):
    collected = []
    for layer_index in range(LAYERS):
        canonical = arrange_whole(joined_weight[layer_index])
        gain_rows = norm_gain[layer_index:layer_index + 1]
        collected.append(finish_tiles(canonical, gain_rows, rotary_order))
    query_weight = jnp.concatenate([item[0] for item in collected], axis=0)
    key_weight = jnp.concatenate([item[1] for item in collected], axis=0)
    value_weight = jnp.concatenate([item[2] for item in collected], axis=0)
    row_peak = jnp.concatenate([item[3] for item in collected], axis=0)
    return query_weight, key_weight, value_weight, row_peak
```

```python
import jax
import jax.numpy as jnp
from jax import lax
from jax.experimental import pallas as pl
from jax.experimental.pallas import tpu as pltpu
from jax.sharding import PartitionSpec as P

HEADS = 32
KV_HEADS = 8
GROUP = 4
SLOTS = GROUP + 2


def pack_kernel(order_ref, stored_ref, out_ref):
    rows = lax.dot_general(
        order_ref[...],
        stored_ref[0],
        (((1,), (1,)), ((), ())),
        preferred_element_type=jnp.float32,
    ).astype(jnp.bfloat16)
    out_ref[...] = rows.reshape(out_ref.shape)


def pack(joined, order, parts, halves):
    layers, features, columns = joined.shape
    width = features // halves
    rows = columns // parts
    return pl.pallas_call(
        pack_kernel,
        grid=(layers, halves),
        in_specs=[
            pl.BlockSpec((columns, columns), lambda l, h: (0, 0)),
            pl.BlockSpec((1, width, columns), lambda l, h: (l, h, 0)),
        ],
        out_specs=pl.BlockSpec((parts, 1, 1, rows, width), lambda l, h: (0, h, l, 0, 0)),
        out_shape=jax.ShapeDtypeStruct((parts, halves, layers, rows, width), joined.dtype),
    )(order, joined)


def finish_kernel(turn_ref, gain_ref, moved_ref, query_ref, key_ref, value_ref, peak_ref):
    gain = gain_ref[0]
    head_dim = turn_ref.shape[0]
    for slot in range(SLOTS):
        tile = moved_ref[:, 0, 0, slot].reshape(head_dim, moved_ref.shape[5])
        if slot <= GROUP:
            tile = jnp.dot(turn_ref[...], tile, preferred_element_type=jnp.float32)
        scaled = (tile.astype(jnp.float32) * gain).astype(jnp.bfloat16)
        if slot < GROUP:
            query_ref[0, slot * head_dim : (slot + 1) * head_dim, :] = scaled
        elif slot == GROUP:
            key_ref[0] = scaled
        else:
            value_ref[0] = scaled
        size = jnp.abs(scaled.astype(jnp.float32))
        step = min(128, size.shape[1])
        top = size[:, :step]
        for start in range(step, size.shape[1], step):
            top = jnp.maximum(top, size[:, start : start + step])
        peak_ref[0, 0, slot : slot + 1, :] = jnp.max(top.T, axis=0, keepdims=True)


def finish(moved, gain, turn):
    sources, layers, groups, slots, piece, width = moved.shape
    head_dim = sources * piece
    return pl.pallas_call(
        finish_kernel,
        grid=(layers, groups),
        in_specs=[
            pl.BlockSpec((head_dim, head_dim), lambda l, g: (0, 0)),
            pl.BlockSpec((1, 1, width), lambda l, g: (l, 0, 0)),
            pl.BlockSpec((sources, 1, 1, slots, piece, width), lambda l, g: (0, l, g, 0, 0, 0)),
        ],
        out_specs=[
            pl.BlockSpec((1, GROUP * head_dim, width), lambda l, g: (l, g, 0)),
            pl.BlockSpec((1, head_dim, width), lambda l, g: (l, g, 0)),
            pl.BlockSpec((1, head_dim, width), lambda l, g: (l, g, 0)),
            pl.BlockSpec((1, 1, slots, head_dim), lambda l, g: (l, g, 0, 0)),
        ],
        out_shape=[
            jax.ShapeDtypeStruct((layers, groups * GROUP * head_dim, width), moved.dtype),
            jax.ShapeDtypeStruct((layers, groups * head_dim, width), moved.dtype),
            jax.ShapeDtypeStruct((layers, groups * head_dim, width), moved.dtype),
            jax.ShapeDtypeStruct((layers, groups, slots, head_dim), jnp.float32),
        ],
    )(turn, gain[:, None, :], moved)


def column_order(columns):
    head_total = HEADS + 2 * KV_HEADS
    piece = columns // head_total
    row = jnp.arange(columns)
    group = row // (SLOTS * piece)
    slot = (row // piece) % SLOTS
    dim = row % piece
    head = jnp.where(
        slot < GROUP,
        group * GROUP + slot,
        jnp.where(slot == GROUP, HEADS + group, HEADS + KV_HEADS + group),
    )
    source = dim * head_total + head
    return (source[:, None] == jnp.arange(columns)[None, :]).astype(jnp.bfloat16)


def solution(mesh):
    parts = mesh.shape["dev"]
    sources = mesh.shape["ma"]

    def shards(joined_weight, norm_gain, rotary_order):
        layers, features, columns = joined_weight.shape
        width = norm_gain.shape[1]
        halves = features // width
        piece = columns // (HEADS + 2 * KV_HEADS)
        packed = pack(joined_weight, column_order(columns), parts, halves)
        grouped = lax.all_to_all(packed, "dev", split_axis=0, concat_axis=0, tiled=True)
        grouped = grouped.reshape(sources, layers, columns // parts, width)
        moved = lax.all_to_all(grouped, "ma", split_axis=0, concat_axis=0, tiled=True)
        moved = moved.reshape(sources, layers, KV_HEADS // parts, SLOTS, piece, width)
        head_dim = rotary_order.shape[0]
        turn = (rotary_order[:, None] == jnp.arange(head_dim)[None, :]).astype(jnp.bfloat16)
        query_rows, key_rows, value_rows, peak = finish(moved, norm_gain, turn)
        row_peak = lax.pmax(peak.reshape(layers, -1), "ma")
        return (query_rows, key_rows, value_rows, row_peak)

    in_specs = (P(None, "dev", "ma"), P(None, "ma"), P())
    out_specs = (P(None, "dev", "ma"), P(None, "dev", "ma"), P(None, "dev", "ma"), P(None, "dev"))
    return jax.shard_map(shards, mesh=mesh, in_specs=in_specs, out_specs=out_specs, check_vma=False)
```
